32 devices in a mesh: head: 2 (over x), outer: 4 (over y, core), inner: 4 (over z).
Axes of the slice: x: 2, y: 2, z: 4, core: 2. Of those that a mesh axis runs over, the one named last changes fastest.
Arguments:
- query_mant: bfloat16 [16, 1024, 128], P('outer', ('head', 'inner')), may hold values from -40 to 40
- key_mant: bfloat16 [1, 1024, 128], P(None, ('head', 'inner')), may hold values from -10 to 10
- value_mant: bfloat16 [1, 1024, 128], P(None, ('head', 'inner')), may hold values from -4 to 4
- out_grad: bfloat16 [16, 1024, 128], P('outer', ('head', 'inner')), may hold values from -4 to 4
- query_exp: int32 [16, 8], P('outer', ('head', 'inner')), may hold values from -1 to 1
- key_exp: int32 [1, 8], P(None, ('head', 'inner')), may hold values from -1 to 1
- value_exp: int32 [1, 8], P(None, ('head', 'inner')), may hold values from -1 to 1
- block_order: int32 [8], replicated, may hold values from 0 to 7, each once
Outputs:
- attended: bfloat16 [16, 1024, 128], P('outer', ('head', 'inner'))
- query_grad: bfloat16 [16, 1024, 128], P('outer', ('head', 'inner'))
- key_grad: bfloat16 [1, 1024, 128], P(None, ('head', 'inner'))
- value_grad: bfloat16 [1, 1024, 128], P(None, ('head', 'inner'))
The draws below stay inside these ranges and needn't reach their ends.
Inputs may be any that keep to these rules, and one draw needn't show every extreme that they name: `block_order`: every number of 0 to 7 once.
All inputs are finite; a program needn't handle non-finite values.
Results may differ from the reference program's by a relative error of at most 0.03.
Values may be sent and summed in bfloat16 or wider, within the bound.
No kernel may reach another device: no remote copies, remote signals or barrier semaphores. Data moves between devices by JAX's collectives and lax.ppermute only.
A program may use at most 64 MiB of HBM per device.

```python
import math
import jax
import jax.numpy as jnp
from jax import lax

HD = 128
GROUP = 16
BLK = 128
HEADS = 16
KV_HEADS = 1
SEQ = 1024
NBLK = 8


def make_keys(key):
    base_keys = jnp.clip(jax.random.normal(jax.random.fold_in(key, 11), (KV_HEADS, SEQ, HD), jnp.float32), -4.0, 4.0)
    keys_all = base_keys
    return keys_all


def draw_key_mant(key, part):
    keys_all = make_keys(key)
    return keys_all.astype(jnp.bfloat16)


def draw_query_mant(key, part):
    drawn = jnp.clip(jax.random.normal(jax.random.fold_in(key, 21), (HEADS, SEQ, HD), jnp.float32), -4.0, 4.0)
    result = drawn
    return result.astype(jnp.bfloat16)


def with_ends(values, key, smallest, top_value):
    longest = values.shape.index(max(values.shape))
    spots = []
    for shift in (0, 1):
        where = [jax.random.randint(jax.random.fold_in(key, axis), (), 0, length) for axis, length in enumerate(values.shape)]
        where[longest] = (where[longest] + shift) % values.shape[longest]
        spots.append(tuple(where))
    return values.at[spots[0]].set(smallest).at[spots[1]].set(top_value)


def block_scale(own_key, extent, cuts, smallest, top_value):
    level, own = 1.0, jax.random.fold_in(own_key, 6)
    for axis_at, shards_of in cuts:
        draws = jnp.exp(jax.random.uniform(jax.random.fold_in(own, axis_at), (shards_of,), jnp.float32, smallest / len(cuts), top_value / len(cuts)))
        level = level * jnp.repeat(draws, extent[axis_at] // shards_of).reshape([-1 if axis == axis_at else 1 for axis in range(len(extent))])
    return level


def gaussian(rng, shape, spread, most, shards=(), held_as=jnp.bfloat16):
    values = jax.random.normal(rng, shape, jnp.float32) * spread
    if len(shards) > 0:
        values = block_scale(rng, shape, shards, -0.22, 0.18) * values
    return jnp.clip(values, min=-most, max=most).astype(held_as)


def setup_inputs(seed: int = 0) -> dict:
    keys = jax.random.split(jax.random.key(seed), 9)
    return {
        "query_mant": draw_query_mant(jax.random.fold_in(keys[8], 71), 0),
        "key_mant": draw_key_mant(jax.random.fold_in(keys[8], 71), 0),
        "value_mant": gaussian(keys[2], (KV_HEADS, SEQ, HD), 1.0, 4.0, ((1, 8),)),
        "out_grad": gaussian(keys[3], (HEADS, SEQ, HD), 1.0, 4.0, ((0, 4), (1, 8))),
        "query_exp": with_ends(jax.random.randint(keys[4], (HEADS, NBLK), -1, 2), jax.random.fold_in(keys[4], 1), -1, 1).astype(jnp.int32),
        "key_exp": with_ends(jax.random.randint(keys[5], (KV_HEADS, NBLK), -1, 2), jax.random.fold_in(keys[5], 1), -1, 1).astype(jnp.int32),
        "value_exp": with_ends(jax.random.randint(keys[6], (KV_HEADS, NBLK), -1, 2), jax.random.fold_in(keys[6], 1), -1, 1).astype(jnp.int32),
        "block_order": jax.random.permutation(keys[7], NBLK).astype(jnp.int32),
    }


def apply_scale(values_in, exps):
    factor = jnp.exp2(exps.astype(jnp.float32))
    factor = jnp.repeat(factor, BLK, axis=1)
    return (values_in.astype(jnp.float32) * factor[:, :, None]).astype(jnp.bfloat16)

def reference(query_mant, key_mant, value_mant, out_grad, query_exp, key_exp, value_exp, block_order):
    width = query_mant.shape[2]
    inv_root = 1.0 / math.sqrt(width)
    row_ids = jnp.arange(SEQ, dtype=jnp.int32)
    token_pos = block_order[row_ids // BLK] * BLK + row_ids % BLK
    visible = token_pos[None, :] <= token_pos[:, None]
    scaled_query = apply_scale(query_mant, query_exp)
    scaled_key = apply_scale(key_mant, key_exp)
    scaled_value = apply_scale(value_mant, value_exp)

    def one_head(index):
        group = (index // GROUP).astype(jnp.int32)
        head_q = lax.dynamic_index_in_dim(scaled_query, index, 0, keepdims=False)
        head_dout = lax.dynamic_index_in_dim(out_grad, index, 0, keepdims=False)
        head_k = lax.dynamic_index_in_dim(scaled_key, group, 0, keepdims=False)
        head_v = lax.dynamic_index_in_dim(scaled_value, group, 0, keepdims=False)
        scores = jnp.dot(head_q, head_k.T, preferred_element_type=jnp.float32) * inv_root
        scores = jnp.where(visible, scores, -1e+30)
        log_total = jax.nn.logsumexp(scores, axis=1)
        probs = jnp.where(visible, jnp.exp(scores - log_total[:, None]), 0.0)
        probs_low = probs.astype(jnp.bfloat16)
        attended = jnp.dot(probs_low, head_v, preferred_element_type=jnp.float32).astype(jnp.bfloat16)
        row_delta = lax.optimization_barrier(jnp.sum(head_dout.astype(jnp.float32) * attended.astype(jnp.float32), axis=1))
        dprob = jnp.dot(head_dout, head_v.T, preferred_element_type=jnp.float32)
        dscore = (probs * (dprob - row_delta[:, None])).astype(jnp.bfloat16)
        grad_q = jnp.dot(dscore, head_k, preferred_element_type=jnp.float32) * inv_root
        grad_k = jnp.dot(dscore.T, head_q, preferred_element_type=jnp.float32) * inv_root
        grad_v = jnp.dot(probs_low.T, head_dout, preferred_element_type=jnp.float32)
        return (attended, grad_q, grad_k, grad_v)
    attended, dq_all, dk_all, dv_all = lax.map(one_head, jnp.arange(HEADS, dtype=jnp.int32))
    q_fac = jnp.repeat(jnp.exp2(query_exp.astype(jnp.float32)), BLK, axis=1)[:, :, None]
    k_fac = jnp.repeat(jnp.exp2(key_exp.astype(jnp.float32)), BLK, axis=1)[:, :, None]
    v_fac = jnp.repeat(jnp.exp2(value_exp.astype(jnp.float32)), BLK, axis=1)[:, :, None]
    query_grad = (dq_all * q_fac).astype(jnp.bfloat16)
    dk_sum = lax.optimization_barrier(jnp.sum(dk_all.reshape(KV_HEADS, GROUP, SEQ, width), axis=1))
    dv_sum = lax.optimization_barrier(jnp.sum(dv_all.reshape(KV_HEADS, GROUP, SEQ, width), axis=1))
    key_grad = (dk_sum * k_fac).astype(jnp.bfloat16)
    value_grad = (dv_sum * v_fac).astype(jnp.bfloat16)
    return (attended, query_grad, key_grad, value_grad)
```

```python
import math

import jax
import jax.numpy as jnp
from jax import lax
from jax.experimental import pallas as pl
from jax.experimental.pallas import tpu as pltpu
from jax.sharding import PartitionSpec as P

GROUP = 16
BLK = 128
ALL = ("head", "outer", "inner")


def scaled(values_in, exps):
    heads, rows, width = values_in.shape
    factor = jnp.exp2(exps.astype(jnp.float32)).astype(jnp.bfloat16)
    blocks = values_in.reshape(heads, rows // BLK, BLK, width) * factor[:, :, None, None]
    return blocks.reshape(heads, rows, width)


def positions(block_order, rows):
    blocks = rows // BLK
    table = jnp.arange(block_order.shape[0], dtype=jnp.int32)
    start = jnp.sum(jnp.where(blocks[:, None] == table[None, :], block_order[None, :], 0), axis=1)
    return start * BLK + rows % BLK


def dot(left, right, left_dim, right_dim):
    return lax.dot_general(
        left, right, (((left_dim,), (right_dim,)), ((), ())), preferred_element_type=jnp.float32
    )


def plan(heads, inners):
    rest = [(h, z) for h in range(heads) for z in range(inners) if (h, z) != (0, 0)]
    steps, own_inverse = [], []
    while rest:
        h, z = rest.pop(0)
        inverse = ((-h) % heads, (-z) % inners)
        if inverse == (h, z):
            own_inverse.append((h, z))
        else:
            rest.remove(inverse)
            steps.append(((h, z), inverse))
    while len(own_inverse) > 1:
        steps.append((own_inverse.pop(), own_inverse.pop()))
    shared = own_inverse[0] if own_inverse else None
    return steps, shared


def moves(sizes, pair, back):
    heads, outers, inners = sizes
    perm = []
    for h in range(heads):
        for o in range(outers):
            for z in range(inners):
                dh, dz = pair[o % 2]
                src = (h * outers + o) * inners + z
                dst = (((h + dh) % heads) * outers + o) * inners + (z + dz) % inners
                perm.append((dst, src) if back else (src, dst))
    return perm


def flip(count, bit):
    return [(o, o ^ bit) for o in range(count)]


def attention_body(parts, factor, seg, starts, row_pos, q, d, *refs):
    pieces = refs[:parts]
    out_ref, dq_ref, own_ref, mine_ref, other_ref = refs[parts : parts + 5]
    kv, p_all, ds_all = refs[parts + 5 :]
    total, wide = kv.shape
    width = wide // 2
    at = 0
    for piece in pieces:
        rows = piece.shape[0]
        kv[at : at + rows, :] = piece[...]
        at += rows
    keys = kv[:, :width]
    values = kv[:, width:]
    count = q.shape[0]
    cols = math.gcd(count, 256)
    key_pos = jnp.concatenate(
        [
            lax.broadcasted_iota(jnp.int32, (seg, 1), 0) + starts[i]
            for i in range(total // seg)
        ],
        axis=0,
    )
    for c in range(0, count, cols):
        span = slice(c, c + cols)
        q_c = q[span, :]
        d_c = d[span, :]
        scores = dot(keys, q_c, 1, 1) * factor
        scores = jnp.where(key_pos <= row_pos[:, span], scores, -1e30)
        best = jnp.max(scores, axis=0, keepdims=True)
        weights = jnp.exp(scores - best)
        total_exp = jnp.sum(weights, axis=0, keepdims=True)
        probs = weights * (1.0 / total_exp)
        probs_low = probs.astype(jnp.bfloat16)
        p_all[:, span] = probs_low
        out_t = dot(values, probs_low, 0, 0)
        out = out_t.T.astype(jnp.bfloat16)
        out_ref[span, :] = out
        d_t = d_c.astype(jnp.float32).T
        delta = jnp.sum(
            d_t * out_t.astype(jnp.bfloat16).astype(jnp.float32), axis=0, keepdims=True
        )
        dprob = dot(values, d_c, 1, 1)
        dscore = (probs * (dprob - delta)).astype(jnp.bfloat16)
        ds_all[:, span] = dscore
        dq_ref[span, :] = (dot(keys, dscore, 0, 0) * factor).T.astype(jnp.bfloat16)
    dk = dot(ds_all[...], q[...], 1, 0) * factor
    dv = dot(p_all[...], d[...], 1, 0)
    own_rows = own_ref.shape[0]
    held = mine_ref.shape[0]
    own_ref[:, :width] = dk[:own_rows]
    own_ref[:, width:] = dv[:own_rows]
    mine_ref[:, :width] = dk[own_rows : own_rows + held]
    mine_ref[:, width:] = dv[own_rows : own_rows + held]
    other_ref[:, :width] = dk[own_rows + held :].astype(jnp.bfloat16)
    other_ref[:, width:] = dv[own_rows + held :].astype(jnp.bfloat16)


def make_on_device(sizes):
    heads_n, outers, inners = sizes
    steps, shared = plan(heads_n, inners)

    def on_device(
        query_mant, key_mant, value_mant, out_grad, query_exp, key_exp, value_exp, block_order
    ):
        heads_out, rows, width = query_mant.shape
        kv_count = key_mant.shape[0]
        wide = 2 * width
        half = rows // 2
        seg = math.gcd(BLK, half)
        count = heads_out * rows
        factor = 1.0 / math.sqrt(width)
        outer_at = lax.axis_index("outer")
        core = outer_at % 2
        head_at = lax.axis_index("head")
        inner_at = lax.axis_index("inner")
        kv_index = outer_at * heads_out // GROUP
        pick = lambda a: lax.dynamic_slice_in_dim(a, kv_index, 1, 0) if kv_count > 1 else a
        block = jnp.concatenate(
            [
                scaled(pick(key_mant), pick(key_exp))[0],
                scaled(pick(value_mant), pick(value_exp))[0],
            ],
            axis=1,
        )
        mine = [lax.ppermute(block, ALL, moves(sizes, pair, False)) for pair in steps]
        if shared is not None:
            part = lax.dynamic_slice_in_dim(block, core * half, half, 0)
            mine.append(lax.ppermute(part, ALL, moves(sizes, (shared, shared), False)))
        other = [lax.ppermute(piece, "outer", flip(outers, 1)) for piece in mine]

        def place_rows(pair, side):
            dh = jnp.where(side == 0, pair[0][0], pair[1][0])
            dz = jnp.where(side == 0, pair[0][1], pair[1][1])
            place = ((head_at - dh) % heads_n) * inners + (inner_at - dz) % inners
            return place * rows

        own_start = (head_at * inners + inner_at) * rows
        firsts = [own_start + i * seg for i in range(rows // seg)]
        for side in (core, 1 - core):
            for pair in steps:
                first = place_rows(pair, side)
                firsts += [first + i * seg for i in range(rows // seg)]
            if shared is not None:
                first = place_rows((shared, shared), side) + side * half
                firsts += [first + i * seg for i in range(half // seg)]
        starts = positions(block_order, jnp.stack(firsts))
        row_pos = jnp.tile(
            positions(block_order, own_start + jnp.arange(rows, dtype=jnp.int32)), heads_out
        )[None]

        pieces = [block] + mine + other
        total = sum(p.shape[0] for p in pieces)
        held = sum(p.shape[0] for p in mine)
        q_scaled = scaled(query_mant, query_exp).reshape(count, width)
        flat_d = out_grad.reshape(count, width)
        vmem = pl.BlockSpec(memory_space=pltpu.VMEM)
        out, dq, own_term, mine_term, other_term = pl.pallas_call(
            lambda *refs: attention_body(len(pieces), factor, seg, *refs),
            in_specs=[pl.BlockSpec(memory_space=pltpu.SMEM)] + [vmem] * (3 + len(pieces)),
            out_specs=[vmem] * 5,
            out_shape=[
                jax.ShapeDtypeStruct((count, width), jnp.bfloat16),
                jax.ShapeDtypeStruct((count, width), jnp.bfloat16),
                jax.ShapeDtypeStruct((rows, wide), jnp.float32),
                jax.ShapeDtypeStruct((held, wide), jnp.float32),
                jax.ShapeDtypeStruct((held, wide), jnp.bfloat16),
            ],
            scratch_shapes=[
                pltpu.VMEM((total, wide), jnp.bfloat16),
                pltpu.VMEM((total, count), jnp.bfloat16),
                pltpu.VMEM((total, count), jnp.bfloat16),
            ],
            name="attention",
        )(starts, row_pos, q_scaled, flat_d, *pieces)
        output = out.reshape(heads_out, rows, width)
        query_grad = scaled(dq.reshape(heads_out, rows, width), query_exp)

        from_core = lax.ppermute(other_term, "outer", flip(outers, 1))
        pair_sum = (mine_term + from_core.astype(jnp.float32)).astype(jnp.bfloat16)
        summed = own_term
        at = 0
        for pair in steps:
            got = lax.ppermute(pair_sum[at : at + rows], ALL, moves(sizes, pair, True))
            summed = summed + got.astype(jnp.float32)
            at += rows
        if shared is not None:
            got = lax.ppermute(
                pair_sum[at : at + half], ALL, moves(sizes, (shared, shared), True)
            ).astype(jnp.float32)
            none = jnp.zeros_like(got)
            low = jnp.concatenate([got, none], axis=0)
            high = jnp.concatenate([none, got], axis=0)
            summed = summed + jnp.where(core == 0, low, high)
        if kv_count == 1 and outers & (outers - 1) == 0:
            bit = outers // 2
            while bit:
                low = summed.astype(jnp.bfloat16)
                got = lax.ppermute(low, "outer", flip(outers, bit))
                summed = low.astype(jnp.float32) + got.astype(jnp.float32)
                bit //= 2
            summed = summed[None]
        else:
            members = lax.all_gather(summed.astype(jnp.bfloat16), "outer", axis=0)
            summed = jnp.sum(
                members.astype(jnp.float32).reshape(kv_count, outers // kv_count, rows, wide),
                axis=1,
            )
        key_grad = scaled(summed[:, :, :width].astype(jnp.bfloat16), key_exp)
        value_grad = scaled(summed[:, :, width:].astype(jnp.bfloat16), value_exp)
        return (output, query_grad, key_grad, value_grad)

    return on_device


def solution(mesh):
    sizes = (mesh.shape["head"], mesh.shape["outer"], mesh.shape["inner"])
    placed = (
        P("outer", ("head", "inner"), None),
        P(None, ("head", "inner"), None),
        P(None, ("head", "inner"), None),
        P("outer", ("head", "inner"), None),
        P("outer", ("head", "inner")),
        P(None, ("head", "inner")),
        P(None, ("head", "inner")),
        P(),
    )
    return jax.shard_map(
        make_on_device(sizes),
        mesh=mesh,
        in_specs=placed,
        out_specs=(
            P("outer", ("head", "inner"), None),
            P("outer", ("head", "inner"), None),
            P(None, ("head", "inner"), None),
            P(None, ("head", "inner"), None),
        ),
        check_vma=False,
    )
```

```python
import math

import jax
import jax.numpy as jnp
from jax import lax
from jax.experimental import pallas as pl
from jax.experimental.pallas import tpu as pltpu
from jax.sharding import PartitionSpec as P

GROUP = 16
BLK = 128
ALL = ("head", "outer", "inner")


def scaled(values_in, exps):
    heads, rows, width = values_in.shape
    factor = jnp.exp2(exps.astype(jnp.float32)).astype(jnp.bfloat16)
    blocks = values_in.reshape(heads, rows // BLK, BLK, width) * factor[:, :, None, None]
    return blocks.reshape(heads, rows, width)


def dot(left, right, left_dim, right_dim):
    return lax.dot_general(
        left, right, (((left_dim,), (right_dim,)), ((), ())), preferred_element_type=jnp.float32
    )


def plan(heads, inners):
    rest = [(h, z) for h in range(heads) for z in range(inners) if (h, z) != (0, 0)]
    steps, own_inverse = [], []
    while rest:
        h, z = rest.pop(0)
        inverse = ((-h) % heads, (-z) % inners)
        if inverse == (h, z):
            own_inverse.append((h, z))
        else:
            rest.remove(inverse)
            steps.append(((h, z), inverse))
    while len(own_inverse) > 1:
        steps.append((own_inverse.pop(), own_inverse.pop()))
    shared = own_inverse[0] if own_inverse else None
    return steps, shared


def moves(sizes, pair, back):
    heads, outers, inners = sizes
    perm = []
    for h in range(heads):
        for o in range(outers):
            for z in range(inners):
                dh, dz = pair[o % 2]
                src = (h * outers + o) * inners + z
                dst = (((h + dh) % heads) * outers + o) * inners + (z + dz) % inners
                perm.append((dst, src) if back else (src, dst))
    return perm


def flip(count, bit):
    return [(o, o ^ bit) for o in range(count)]


def place_start(sizes, pair, side, rows):
    heads_n, _, inners = sizes
    dh = jnp.where(side == 0, pair[0][0], pair[1][0])
    dz = jnp.where(side == 0, pair[0][1], pair[1][1])
    h = lax.axis_index("head") + (heads_n - dh)
    z = lax.axis_index("inner") + (inners - dz)
    h = jnp.where(h >= heads_n, h - heads_n, h)
    z = jnp.where(z >= inners, z - inners, z)
    return (h * inners + z) * rows


def power(exps, width):
    return jnp.exp2(jnp.full((1, width), exps, jnp.int32).astype(jnp.float32))


def block_body(share, key_hbm, value_hbm, kexp_hbm, vexp_hbm, *refs):
    outs = refs[: 1 + share]
    keys, values, kexp, vexp, sems = refs[1 + share :]
    copies = [
        pltpu.make_async_copy(src, dst, sems.at[i])
        for i, (src, dst) in enumerate(
            ((key_hbm, keys), (value_hbm, values), (kexp_hbm, kexp), (vexp_hbm, vexp))
        )
    ]
    for copy in copies:
        copy.start()
    for copy in copies:
        copy.wait()
    rows, width = keys.shape[1:]
    for src, exps, at in ((keys, kexp, 0), (values, vexp, width)):
        for b in range(rows // BLK):
            span = slice(b * BLK, (b + 1) * BLK)
            wide = src[0, span, :].astype(jnp.float32) * power(exps[0, b], width)
            outs[0][span, at : at + width] = wide.astype(jnp.bfloat16)
    if share:
        core = lax.axis_index("outer") % 2
        half = rows // 2
        outs[1][...] = jnp.where(core == 0, outs[0][:half, :], outs[0][half:, :])


def attention_body(sizes, steps, shared, rows, parts, order, qexp, q_in, d, *refs):
    pieces = refs[:parts]
    out_ref, dq_ref, own_ref, mine_ref, other_ref = refs[parts : parts + 5]
    kv, q, p_all, ds_all = refs[parts + 5 :]
    total, wide = kv.shape
    width = wide // 2
    count = q.shape[0]
    half = rows // 2
    seg = math.gcd(BLK, half)
    factor = 1.0 / math.sqrt(width)
    core = lax.axis_index("outer") % 2
    at = 0
    for piece in pieces:
        have = piece.shape[0]
        kv[at : at + have, :] = piece[...]
        at += have
    blocks = rows // BLK
    for i in range(count // BLK):
        span = slice(i * BLK, (i + 1) * BLK)
        scale = power(qexp[i // blocks, i % blocks], width)
        q[span, :] = (q_in[span, :].astype(jnp.float32) * scale).astype(jnp.bfloat16)
    own_start = (lax.axis_index("head") * sizes[2] + lax.axis_index("inner")) * rows
    firsts = [own_start + i * seg for i in range(rows // seg)]
    for side in (core, 1 - core):
        for pair in steps:
            first = place_start(sizes, pair, side, rows)
            firsts += [first + i * seg for i in range(rows // seg)]
        if shared is not None:
            first = place_start(sizes, (shared, shared), side, rows) + side * half
            firsts += [first + i * seg for i in range(half // seg)]
    keys = kv[:, :width]
    values = kv[:, width:]
    cols = math.gcd(count, 256)
    shift = BLK.bit_length() - 1
    key_pos = jnp.concatenate(
        [
            lax.broadcasted_iota(jnp.int32, (seg, 1), 0)
            + (order[lax.shift_right_logical(f, shift)] * BLK + (f & (BLK - 1)))
            for f in firsts
        ],
        axis=0,
    )
    own_block = lax.shift_right_logical(own_start, shift)
    for c in range(0, count, cols):
        span = slice(c, c + cols)
        q_c = q[span, :]
        d_c = d[span, :]
        row_pos = jnp.concatenate(
            [
                lax.broadcasted_iota(jnp.int32, (1, BLK), 1)
                + order[own_block + (i % blocks)] * BLK
                for i in range(c // BLK, (c + cols) // BLK)
            ],
            axis=1,
        )
        scores = dot(keys, q_c, 1, 1) * (factor * math.log2(math.e))
        scores = jnp.where(key_pos <= row_pos, scores, -1e30)
        best = jnp.max(scores, axis=0, keepdims=True)
        weights = jnp.exp2(scores - best)
        total_exp = jnp.sum(weights, axis=0, keepdims=True)
        probs = weights * (1.0 / total_exp)
        probs_low = probs.astype(jnp.bfloat16)
        p_all[:, span] = probs_low
        out_t = dot(values, probs_low, 0, 0)
        out_ref[span, :] = out_t.T.astype(jnp.bfloat16)
        d_t = d_c.astype(jnp.float32).T
        delta = jnp.sum(
            d_t * out_t.astype(jnp.bfloat16).astype(jnp.float32), axis=0, keepdims=True
        )
        dprob = dot(values, d_c, 1, 1)
        dscore = (probs * (dprob - delta)).astype(jnp.bfloat16)
        ds_all[:, span] = dscore
        dq = (dot(keys, dscore, 0, 0) * factor).T
        for i in range(cols // BLK):
            g = c // BLK + i
            scale = power(qexp[g // blocks, g % blocks], width)
            dq_ref[g * BLK : (g + 1) * BLK, :] = (
                dq[i * BLK : (i + 1) * BLK] * scale
            ).astype(jnp.bfloat16)
    dk = dot(ds_all[...], q[...], 1, 0) * factor
    dv = dot(p_all[...], d[...], 1, 0)
    held = mine_ref.shape[0]
    own_ref[:, :width] = dk[:rows]
    own_ref[:, width:] = dv[:rows]
    mine_ref[:, :width] = dk[rows : rows + held]
    mine_ref[:, width:] = dv[rows : rows + held]
    other_ref[:, :width] = dk[rows + held :].astype(jnp.bfloat16)
    other_ref[:, width:] = dv[rows + held :].astype(jnp.bfloat16)


def pair_body(mine, other, *outs):
    at = 0
    for out in outs:
        span = slice(at, at + out.shape[0])
        out[...] = (mine[span, :] + other[span, :].astype(jnp.float32)).astype(jnp.bfloat16)
        at += out.shape[0]


def final_body(count, kexp, vexp, *refs):
    terms = [ref[...].astype(jnp.float32) for ref in refs[:count]]
    while len(terms) > 1:
        terms = [terms[i] + terms[i + 1] for i in range(0, len(terms), 2)]
    key_out, value_out = refs[count:]
    rows, width = key_out.shape[1:]
    for out, exps, at in ((key_out, kexp, 0), (value_out, vexp, width)):
        for b in range(rows // BLK):
            span = slice(b * BLK, (b + 1) * BLK)
            out[0, span, :] = (
                terms[0][span, at : at + width] * power(exps[0, b], width)
            ).astype(jnp.bfloat16)


def make_on_device(sizes):
    heads_n, outers, inners = sizes
    steps, shared = plan(heads_n, inners)
    vmem = pl.BlockSpec(memory_space=pltpu.VMEM)
    smem = pl.BlockSpec(memory_space=pltpu.SMEM)
    hbm = pl.BlockSpec(memory_space=pl.ANY)

    def on_device(
        query_mant, key_mant, value_mant, out_grad, query_exp, key_exp, value_exp, block_order
    ):
        heads_out, rows, width = query_mant.shape
        kv_count = key_mant.shape[0]
        wide = 2 * width
        half = rows // 2
        count = heads_out * rows
        outer_at = lax.axis_index("outer")
        core = outer_at % 2
        kv_index = outer_at * heads_out // GROUP
        pick = lambda a: lax.dynamic_slice_in_dim(a, kv_index, 1, 0) if kv_count > 1 else a
        share = 0 if shared is None else 1
        block, *part = pl.pallas_call(
            lambda *refs: block_body(share, *refs),
            in_specs=[hbm] * 4,
            out_specs=[vmem] * (1 + share),
            out_shape=[
                jax.ShapeDtypeStruct((size, wide), jnp.bfloat16) for size in (rows, half)
            ][: 1 + share],
            scratch_shapes=[
                pltpu.VMEM((1, rows, width), jnp.bfloat16),
                pltpu.VMEM((1, rows, width), jnp.bfloat16),
                pltpu.SMEM((1, rows // BLK), jnp.int32),
                pltpu.SMEM((1, rows // BLK), jnp.int32),
                pltpu.SemaphoreType.DMA((4,)),
            ],
            name="scale_block",
        )(pick(key_mant), pick(value_mant), pick(key_exp), pick(value_exp))
        mine = [lax.ppermute(block, ALL, moves(sizes, pair, False)) for pair in steps]
        if share:
            mine.append(lax.ppermute(part[0], ALL, moves(sizes, (shared, shared), False)))
        other = [lax.ppermute(piece, "outer", flip(outers, 1)) for piece in mine]

        pieces = [block] + mine + other
        total = sum(p.shape[0] for p in pieces)
        held = sum(p.shape[0] for p in mine)
        out, dq, own_term, mine_term, other_term = pl.pallas_call(
            lambda *refs: attention_body(sizes, steps, shared, rows, len(pieces), *refs),
            in_specs=[smem, smem] + [vmem] * (2 + len(pieces)),
            out_specs=[vmem] * 5,
            out_shape=[
                jax.ShapeDtypeStruct((count, width), jnp.bfloat16),
                jax.ShapeDtypeStruct((count, width), jnp.bfloat16),
                jax.ShapeDtypeStruct((rows, wide), jnp.float32),
                jax.ShapeDtypeStruct((held, wide), jnp.float32),
                jax.ShapeDtypeStruct((held, wide), jnp.bfloat16),
            ],
            scratch_shapes=[
                pltpu.VMEM((total, wide), jnp.bfloat16),
                pltpu.VMEM((count, width), jnp.bfloat16),
                pltpu.VMEM((total, count), jnp.bfloat16),
                pltpu.VMEM((total, count), jnp.bfloat16),
            ],
            name="attention",
        )(
            block_order,
            query_exp,
            query_mant.reshape(count, width),
            out_grad.reshape(count, width),
            *pieces,
        )
        output = out.reshape(heads_out, rows, width)
        query_grad = dq.reshape(heads_out, rows, width)

        from_core = lax.ppermute(other_term, "outer", flip(outers, 1))
        pair_sums = pl.pallas_call(
            pair_body,
            in_specs=[vmem] * 2,
            out_specs=[vmem] * len(mine),
            out_shape=[jax.ShapeDtypeStruct(p.shape, jnp.bfloat16) for p in mine],
            name="pair_sum",
        )(mine_term, from_core)
        summed = own_term
        for pair, piece in zip(steps, pair_sums):
            got = lax.ppermute(piece, ALL, moves(sizes, pair, True))
            summed = summed + got.astype(jnp.float32)
        if share:
            got = lax.ppermute(
                pair_sums[-1], ALL, moves(sizes, (shared, shared), True)
            ).astype(jnp.float32)
            none = jnp.zeros_like(got)
            low = jnp.concatenate([got, none], axis=0)
            high = jnp.concatenate([none, got], axis=0)
            summed = summed + jnp.where(core == 0, low, high)
        low = summed.astype(jnp.bfloat16)
        if kv_count == 1 and outers & (outers - 1) == 0:
            terms = [low] + [lax.ppermute(low, "outer", flip(outers, m)) for m in range(1, outers)]
            grad = jax.ShapeDtypeStruct((1, rows, width), jnp.bfloat16)
            key_grad, value_grad = pl.pallas_call(
                lambda *refs: final_body(outers, *refs),
                in_specs=[smem, smem] + [vmem] * outers,
                out_specs=[vmem] * 2,
                out_shape=[grad, grad],
                name="final_sum",
            )(key_exp, value_exp, *terms)
            return (output, query_grad, key_grad, value_grad)
        members = lax.all_gather(low, "outer", axis=0)
        summed = jnp.sum(
            members.astype(jnp.float32).reshape(kv_count, outers // kv_count, rows, wide), axis=1
        )
        key_grad = scaled(summed[:, :, :width].astype(jnp.bfloat16), key_exp)
        value_grad = scaled(summed[:, :, width:].astype(jnp.bfloat16), value_exp)
        return (output, query_grad, key_grad, value_grad)

    return on_device


def solution(mesh):
    sizes = (mesh.shape["head"], mesh.shape["outer"], mesh.shape["inner"])
    placed = (
        P("outer", ("head", "inner"), None),
        P(None, ("head", "inner"), None),
        P(None, ("head", "inner"), None),
        P("outer", ("head", "inner"), None),
        P("outer", ("head", "inner")),
        P(None, ("head", "inner")),
        P(None, ("head", "inner")),
        P(),
    )
    return jax.shard_map(
        make_on_device(sizes),
        mesh=mesh,
        in_specs=placed,
        out_specs=(
            P("outer", ("head", "inner"), None),
            P("outer", ("head", "inner"), None),
            P(None, ("head", "inner"), None),
            P(None, ("head", "inner"), None),
        ),
        check_vma=False,
    )
```

```python
import math

import jax
import jax.numpy as jnp
from jax import lax
from jax.experimental import pallas as pl
from jax.experimental.pallas import tpu as pltpu
from jax.sharding import PartitionSpec as P

GROUP = 16
BLK = 128
ALL = ("head", "outer", "inner")


def scaled(values_in, exps):
    heads, rows, width = values_in.shape
    factor = jnp.exp2(exps.astype(jnp.float32)).astype(jnp.bfloat16)
    blocks = values_in.reshape(heads, rows // BLK, BLK, width) * factor[:, :, None, None]
    return blocks.reshape(heads, rows, width)


def dot(left, right, left_dim, right_dim):
    return lax.dot_general(
        left, right, (((left_dim,), (right_dim,)), ((), ())), preferred_element_type=jnp.float32
    )


def plan(heads, inners):
    rest = [(h, z) for h in range(heads) for z in range(inners) if (h, z) != (0, 0)]
    steps, own_inverse = [], []
    while rest:
        h, z = rest.pop(0)
        inverse = ((-h) % heads, (-z) % inners)
        if inverse == (h, z):
            own_inverse.append((h, z))
        else:
            rest.remove(inverse)
            steps.append(((h, z), inverse))
    while len(own_inverse) > 1:
        steps.append((own_inverse.pop(), own_inverse.pop()))
    shared = own_inverse[0] if own_inverse else None
    return steps, shared


def moves(sizes, pair, back):
    heads, outers, inners = sizes
    perm = []
    for h in range(heads):
        for o in range(outers):
            for z in range(inners):
                dh, dz = pair[o % 2]
                src = (h * outers + o) * inners + z
                dst = (((h + dh) % heads) * outers + o) * inners + (z + dz) % inners
                perm.append((dst, src) if back else (src, dst))
    return perm


def flip(count, bit):
    return [(o, o ^ bit) for o in range(count)]


def place_start(sizes, pair, side, rows):
    heads_n, _, inners = sizes
    dh = jnp.where(side == 0, pair[0][0], pair[1][0])
    dz = jnp.where(side == 0, pair[0][1], pair[1][1])
    h = lax.axis_index("head") + (heads_n - dh)
    z = lax.axis_index("inner") + (inners - dz)
    h = jnp.where(h >= heads_n, h - heads_n, h)
    z = jnp.where(z >= inners, z - inners, z)
    return (h * inners + z) * rows


def power(exps, width):
    return jnp.exp2(jnp.full((1, width), exps, jnp.int32).astype(jnp.float32))


def block_body(share, key_hbm, value_hbm, exp_hbm, *refs):
    block, factors = refs[:2]
    keys, values, exps, sems = refs[2 + share :]
    copies = [
        pltpu.make_async_copy(src, dst, sems.at[i])
        for i, (src, dst) in enumerate(
            ((key_hbm, keys), (value_hbm, values), (exp_hbm, exps))
        )
    ]
    for copy in copies:
        copy.start()
    for copy in copies:
        copy.wait()
    rows, width = keys.shape[1:]
    blocks = rows // BLK
    for src, first, at in ((keys, 0, 0), (values, blocks, width)):
        for b in range(blocks):
            span = slice(b * BLK, (b + 1) * BLK)
            factor = jnp.exp2(exps[first + b : first + b + 1, :].astype(jnp.float32))
            factors[b : b + 1, at : at + width] = factor
            wide = src[0, span, :].astype(jnp.float32) * factor
            block[span, at : at + width] = wide.astype(jnp.bfloat16)
    if share:
        core = lax.axis_index("outer") % 2
        half = rows // 2
        refs[2][...] = jnp.where(core == 0, block[:half, :], block[half:, :])


def attention_body(sizes, steps, shared, rows, parts, *refs):
    sources = refs[:4]
    pieces = refs[4 : 4 + parts]
    out_ref, dq_ref, own_ref = refs[4 + parts : 7 + parts]
    at = 7 + parts + len(steps) + (0 if shared is None else 1)
    mine_refs = refs[7 + parts : at]
    other_ref = refs[at]
    order, qexp, q_in, d, sems, kv, q, p_all, ds_all = refs[at + 1 :]
    copies = [
        pltpu.make_async_copy(src, dst, sems.at[i])
        for i, (src, dst) in enumerate(zip(sources, (order, qexp, q_in, d)))
    ]
    for copy in copies:
        copy.start()
    total, wide = kv.shape
    width = wide // 2
    count = q.shape[0]
    half = rows // 2
    seg = math.gcd(BLK, half)
    factor = 1.0 / math.sqrt(width)
    core = lax.axis_index("outer") % 2
    at = 0
    for piece in pieces:
        have = piece.shape[0]
        kv[at : at + have, :] = piece[...]
        at += have
    for copy in copies:
        copy.wait()
    blocks = rows // BLK
    for i in range(count // BLK):
        span = slice(i * BLK, (i + 1) * BLK)
        scale = power(qexp[i % blocks, i // blocks], width)
        q[span, :] = (q_in[span, :].astype(jnp.float32) * scale).astype(jnp.bfloat16)
    own_start = (lax.axis_index("head") * sizes[2] + lax.axis_index("inner")) * rows
    firsts = [own_start + i * seg for i in range(rows // seg)]
    for side in (core, 1 - core):
        for pair in steps:
            first = place_start(sizes, pair, side, rows)
            firsts += [first + i * seg for i in range(rows // seg)]
        if shared is not None:
            first = place_start(sizes, (shared, shared), side, rows) + side * half
            firsts += [first + i * seg for i in range(half // seg)]
    keys = kv[:, :width]
    values = kv[:, width:]
    cols = math.gcd(count, 256)
    shift = BLK.bit_length() - 1
    key_pos = jnp.concatenate(
        [
            lax.broadcasted_iota(jnp.int32, (seg, 1), 0)
            + (order[lax.shift_right_logical(f, shift)] * BLK + (f & (BLK - 1)))
            for f in firsts
        ],
        axis=0,
    )
    own_block = lax.shift_right_logical(own_start, shift)
    for c in range(0, count, cols):
        span = slice(c, c + cols)
        q_c = q[span, :]
        d_c = d[span, :]
        row_pos = jnp.concatenate(
            [
                lax.broadcasted_iota(jnp.int32, (1, BLK), 1)
                + order[own_block + (i % blocks)] * BLK
                for i in range(c // BLK, (c + cols) // BLK)
            ],
            axis=1,
        )
        scores = dot(keys, q_c, 1, 1) * (factor * math.log2(math.e))
        scores = jnp.where(key_pos <= row_pos, scores, -1e30)
        best = jnp.max(scores, axis=0, keepdims=True)
        weights = jnp.exp2(scores - best)
        total_exp = jnp.sum(weights, axis=0, keepdims=True)
        probs = weights * (1.0 / total_exp)
        probs_low = probs.astype(jnp.bfloat16)
        p_all[:, span] = probs_low
        out_t = dot(values, probs_low, 0, 0)
        out_ref[span, :] = out_t.T.astype(jnp.bfloat16)
        d_t = d_c.astype(jnp.float32).T
        delta = jnp.sum(
            d_t * out_t.astype(jnp.bfloat16).astype(jnp.float32), axis=0, keepdims=True
        )
        dprob = dot(values, d_c, 1, 1)
        dscore = (probs * (dprob - delta)).astype(jnp.bfloat16)
        ds_all[:, span] = dscore
        dq = (dot(keys, dscore, 0, 0) * factor).T
        for i in range(cols // BLK):
            g = c // BLK + i
            scale = power(qexp[g % blocks, g // blocks], width)
            dq_ref[g * BLK : (g + 1) * BLK, :] = (
                dq[i * BLK : (i + 1) * BLK] * scale
            ).astype(jnp.bfloat16)
    dk = dot(ds_all[...], q[...], 1, 0) * factor
    dv = dot(p_all[...], d[...], 1, 0)
    own_ref[:, :width] = dk[:rows]
    own_ref[:, width:] = dv[:rows]
    at = rows
    for mine_ref in mine_refs:
        end = at + mine_ref.shape[0]
        mine_ref[:, :width] = dk[at:end]
        mine_ref[:, width:] = dv[at:end]
        at = end
    other_ref[:, :width] = dk[at:].astype(jnp.bfloat16)
    other_ref[:, width:] = dv[at:].astype(jnp.bfloat16)


def make_on_device(sizes):
    heads_n, outers, inners = sizes
    steps, shared = plan(heads_n, inners)
    vmem = pl.BlockSpec(memory_space=pltpu.VMEM)
    hbm = pl.BlockSpec(memory_space=pltpu.HBM)
    keep = lambda a: pltpu.with_memory_space_constraint(a, pltpu.VMEM)
    stay = lambda a: pltpu.with_memory_space_constraint(a, pltpu.HBM)
    params = pltpu.CompilerParams(vmem_limit_bytes=24 * 1024 * 1024)

    def on_device(
        query_mant, key_mant, value_mant, out_grad, query_exp, key_exp, value_exp, block_order
    ):
        heads_out, rows, width = query_mant.shape
        kv_count = key_mant.shape[0]
        wide = 2 * width
        half = rows // 2
        count = heads_out * rows
        outer_at = lax.axis_index("outer")
        core = outer_at % 2
        kv_index = outer_at * heads_out // GROUP
        pick = lambda a: lax.dynamic_slice_in_dim(a, kv_index, 1, 0) if kv_count > 1 else a
        share = 0 if shared is None else 1
        exps = jnp.concatenate([pick(key_exp)[0], pick(value_exp)[0]])
        exps = jnp.broadcast_to(exps[:, None], (exps.shape[0], width))
        block, factors, *part = pl.pallas_call(
            lambda *refs: block_body(share, *refs),
            in_specs=[hbm] * 3,
            out_specs=[vmem] * (2 + share),
            out_shape=[
                pltpu.VMEM((rows, wide), jnp.bfloat16),
                pltpu.VMEM((rows // BLK, wide), jnp.float32),
                pltpu.VMEM((half, wide), jnp.bfloat16),
            ][: 2 + share],
            scratch_shapes=[
                pltpu.VMEM((1, rows, width), jnp.bfloat16),
                pltpu.VMEM((1, rows, width), jnp.bfloat16),
                pltpu.VMEM((2 * (rows // BLK), width), jnp.int32),
                pltpu.SemaphoreType.DMA((3,)),
            ],
            compiler_params=params,
            name="scale_block",
        )(stay(pick(key_mant)), stay(pick(value_mant)), stay(exps))
        mine = [lax.ppermute(block, ALL, moves(sizes, pair, False)) for pair in steps]
        if share:
            mine.append(lax.ppermute(part[0], ALL, moves(sizes, (shared, shared), False)))
        other = [lax.ppermute(piece, "outer", flip(outers, 1)) for piece in mine]

        pieces = [block] + mine + other
        total = sum(p.shape[0] for p in pieces)
        held = sum(p.shape[0] for p in mine)
        out, dq, own_term, *mine_terms, other_term = pl.pallas_call(
            lambda *refs: attention_body(sizes, steps, shared, rows, len(pieces), *refs),
            in_specs=[hbm] * 4 + [vmem] * len(pieces),
            out_specs=[vmem] * (4 + len(mine)),
            out_shape=[
                jax.ShapeDtypeStruct((count, width), jnp.bfloat16),
                jax.ShapeDtypeStruct((count, width), jnp.bfloat16),
                pltpu.VMEM((rows, wide), jnp.float32),
            ]
            + [pltpu.VMEM(p.shape, jnp.float32) for p in mine]
            + [pltpu.VMEM((held, wide), jnp.bfloat16)],
            scratch_shapes=[
                pltpu.SMEM(block_order.shape, jnp.int32),
                pltpu.SMEM((rows // BLK, heads_out), jnp.int32),
                pltpu.VMEM((count, width), jnp.bfloat16),
                pltpu.VMEM((count, width), jnp.bfloat16),
                pltpu.SemaphoreType.DMA((4,)),
                pltpu.VMEM((total, wide), jnp.bfloat16),
                pltpu.VMEM((count, width), jnp.bfloat16),
                pltpu.VMEM((total, count), jnp.bfloat16),
                pltpu.VMEM((total, count), jnp.bfloat16),
            ],
            compiler_params=pltpu.CompilerParams(vmem_limit_bytes=48 * 1024 * 1024),
            name="attention",
        )(
            stay(block_order),
            stay(query_exp.T),
            stay(query_mant.reshape(count, width)),
            stay(out_grad.reshape(count, width)),
            *[keep(piece) for piece in pieces],
        )
        output = out.reshape(heads_out, rows, width)
        query_grad = dq.reshape(heads_out, rows, width)

        from_core = lax.ppermute(other_term, "outer", flip(outers, 1))
        pair_sums = []
        at = 0
        for term in mine_terms:
            end = at + term.shape[0]
            pair_sums.append((term + from_core[at:end].astype(jnp.float32)).astype(jnp.bfloat16))
            at = end
        summed = own_term
        for pair, piece in zip(steps, pair_sums):
            got = lax.ppermute(piece, ALL, moves(sizes, pair, True))
            summed = summed + got.astype(jnp.float32)
        if share:
            got = lax.ppermute(
                pair_sums[-1], ALL, moves(sizes, (shared, shared), True)
            ).astype(jnp.float32)
            none = jnp.zeros_like(got)
            low = jnp.concatenate([got, none], axis=0)
            high = jnp.concatenate([none, got], axis=0)
            summed = summed + jnp.where(core == 0, low, high)
        low = summed.astype(jnp.bfloat16)
        if kv_count == 1 and outers & (outers - 1) == 0:
            bit = outers // 2
            while bit:
                got = lax.ppermute(low, "outer", flip(outers, bit))
                summed = low.astype(jnp.float32) + got.astype(jnp.float32)
                low = summed.astype(jnp.bfloat16)
                bit //= 2
            grads = [
                (
                    summed[:, at : at + width].reshape(rows // BLK, BLK, width)
                    * factors[:, None, at : at + width]
                )
                .astype(jnp.bfloat16)
                .reshape(1, rows, width)
                for at in (0, width)
            ]
            return (output, query_grad, grads[0], grads[1])
        members = lax.all_gather(low, "outer", axis=0)
        summed = jnp.sum(
            members.astype(jnp.float32).reshape(kv_count, outers // kv_count, rows, wide), axis=1
        )
        key_grad = scaled(summed[:, :, :width].astype(jnp.bfloat16), key_exp)
        value_grad = scaled(summed[:, :, width:].astype(jnp.bfloat16), value_exp)
        return (output, query_grad, key_grad, value_grad)

    return on_device


def solution(mesh):
    sizes = (mesh.shape["head"], mesh.shape["outer"], mesh.shape["inner"])
    placed = (
        P("outer", ("head", "inner"), None),
        P(None, ("head", "inner"), None),
        P(None, ("head", "inner"), None),
        P("outer", ("head", "inner"), None),
        P("outer", ("head", "inner")),
        P(None, ("head", "inner")),
        P(None, ("head", "inner")),
        P(),
    )
    return jax.shard_map(
        make_on_device(sizes),
        mesh=mesh,
        in_specs=placed,
        out_specs=(
            P("outer", ("head", "inner"), None),
            P("outer", ("head", "inner"), None),
            P(None, ("head", "inner"), None),
            P(None, ("head", "inner"), None),
        ),
        check_vma=False,
    )
```

```python
import math

import jax
import jax.numpy as jnp
from jax import lax
from jax.experimental import pallas as pl
from jax.experimental.pallas import tpu as pltpu
from jax.sharding import PartitionSpec as P

GROUP = 16
BLK = 128
ALL = ("head", "outer", "inner")


def scaled(values_in, exps):
    heads, rows, width = values_in.shape
    factor = jnp.exp2(exps.astype(jnp.float32)).astype(jnp.bfloat16)
    blocks = values_in.reshape(heads, rows // BLK, BLK, width) * factor[:, :, None, None]
    return blocks.reshape(heads, rows, width)


def dot(left, right, left_dim, right_dim):
    return lax.dot_general(
        left, right, (((left_dim,), (right_dim,)), ((), ())), preferred_element_type=jnp.float32
    )


def plan(heads, inners):
    rest = [(h, z) for h in range(heads) for z in range(inners) if (h, z) != (0, 0)]
    steps, own_inverse = [], []
    while rest:
        h, z = rest.pop(0)
        inverse = ((-h) % heads, (-z) % inners)
        if inverse == (h, z):
            own_inverse.append((h, z))
        else:
            rest.remove(inverse)
            steps.append(((h, z), inverse))
    while len(own_inverse) > 1:
        steps.append((own_inverse.pop(), own_inverse.pop()))
    shared = own_inverse[0] if own_inverse else None
    steps.reverse()
    return steps, shared


def moves(sizes, pair, back):
    heads, outers, inners = sizes
    perm = []
    for h in range(heads):
        for o in range(outers):
            for z in range(inners):
                dh, dz = pair[o % 2]
                src = (h * outers + o) * inners + z
                dst = (((h + dh) % heads) * outers + o) * inners + (z + dz) % inners
                perm.append((dst, src) if back else (src, dst))
    return perm


def flip(count, bit):
    return [(o, o ^ bit) for o in range(count)]


def place_start(sizes, pair, side, rows):
    heads_n, _, inners = sizes
    dh = jnp.where(side == 0, pair[0][0], pair[1][0])
    dz = jnp.where(side == 0, pair[0][1], pair[1][1])
    h = lax.axis_index("head") + (heads_n - dh)
    z = lax.axis_index("inner") + (inners - dz)
    h = jnp.where(h >= heads_n, h - heads_n, h)
    z = jnp.where(z >= inners, z - inners, z)
    return (h * inners + z) * rows


def power(exps, width):
    return jnp.exp2(jnp.full((1, width), exps, jnp.int32).astype(jnp.float32))


def block_body(share, key_hbm, value_hbm, exp_hbm, *refs):
    block, factors = refs[:2]
    keys, values, exps, sems = refs[2 + share :]
    copies = [
        pltpu.make_async_copy(src, dst, sems.at[i])
        for i, (src, dst) in enumerate(
            ((key_hbm, keys), (value_hbm, values), (exp_hbm, exps))
        )
    ]
    for copy in copies:
        copy.start()
    for copy in copies:
        copy.wait()
    rows, width = keys.shape[1:]
    blocks = rows // BLK
    for src, first, at in ((keys, 0, 0), (values, 1, width)):
        for b in range(blocks):
            span = slice(b * BLK, (b + 1) * BLK)
            power_of = jnp.exp2(exps[first : first + 1, b : b + 1].astype(jnp.float32))
            factor = jnp.broadcast_to(power_of, (1, width))
            factors[b : b + 1, at : at + width] = factor
            wide = src[0, span, :].astype(jnp.float32) * factor
            block[span, at : at + width] = wide.astype(jnp.bfloat16)
    if share:
        core = lax.axis_index("outer") % 2
        half = rows // 2
        refs[2][...] = jnp.where(core == 0, block[:half, :], block[half:, :])


def attention_body(sizes, steps, shared, rows, parts, *refs):
    sources = refs[:4]
    pieces = refs[4 : 4 + parts]
    out_ref, dq_ref, own_ref = refs[4 + parts : 7 + parts]
    at = 7 + parts + len(steps) + (0 if shared is None else 1)
    mine_refs = refs[7 + parts : at]
    other_ref = refs[at]
    order, qexp, q_in, d, sems, kv, q, p_all, ds_all = refs[at + 1 :]
    copies = [
        pltpu.make_async_copy(src, dst, sems.at[i])
        for i, (src, dst) in enumerate(zip(sources, (order, qexp, q_in, d)))
    ]
    for copy in copies:
        copy.start()
    total, wide = kv.shape
    width = wide // 2
    count = q.shape[0]
    half = rows // 2
    seg = math.gcd(BLK, half)
    factor = 1.0 / math.sqrt(width)
    core = lax.axis_index("outer") % 2
    at = 0
    for piece in pieces:
        have = piece.shape[0]
        kv[at : at + have, :] = piece[...]
        at += have
    for copy in copies:
        copy.wait()
    blocks = rows // BLK
    for i in range(count // BLK):
        span = slice(i * BLK, (i + 1) * BLK)
        scale = power(qexp[i % blocks, i // blocks], width)
        q[span, :] = (q_in[span, :].astype(jnp.float32) * scale).astype(jnp.bfloat16)
    own_start = (lax.axis_index("head") * sizes[2] + lax.axis_index("inner")) * rows
    firsts = [own_start + i * seg for i in range(rows // seg)]
    for side in (core, 1 - core):
        for pair in steps:
            first = place_start(sizes, pair, side, rows)
            firsts += [first + i * seg for i in range(rows // seg)]
        if shared is not None:
            first = place_start(sizes, (shared, shared), side, rows) + side * half
            firsts += [first + i * seg for i in range(half // seg)]
    keys = kv[:, :width]
    values = kv[:, width:]
    cols = math.gcd(count, 256)
    shift = BLK.bit_length() - 1
    key_pos = jnp.concatenate(
        [
            lax.broadcasted_iota(jnp.int32, (seg, 1), 0)
            + (order[lax.shift_right_logical(f, shift)] * BLK + (f & (BLK - 1)))
            for f in firsts
        ],
        axis=0,
    )
    own_block = lax.shift_right_logical(own_start, shift)
    for c in range(0, count, cols):
        span = slice(c, c + cols)
        q_c = q[span, :]
        d_c = d[span, :]
        row_pos = jnp.concatenate(
            [
                lax.broadcasted_iota(jnp.int32, (1, BLK), 1)
                + order[own_block + (i % blocks)] * BLK
                for i in range(c // BLK, (c + cols) // BLK)
            ],
            axis=1,
        )
        scores = dot(keys, q_c, 1, 1) * (factor * math.log2(math.e))
        scores = jnp.where(key_pos <= row_pos, scores, -1e30)
        best = jnp.max(scores, axis=0, keepdims=True)
        weights = jnp.exp2(scores - best)
        total_exp = jnp.sum(weights, axis=0, keepdims=True)
        probs = weights * (1.0 / total_exp)
        probs_low = probs.astype(jnp.bfloat16)
        p_all[:, span] = probs_low
        out_t = dot(values, probs_low, 0, 0)
        out_ref[span, :] = out_t.T.astype(jnp.bfloat16)
        d_t = d_c.astype(jnp.float32).T
        delta = jnp.sum(
            d_t * out_t.astype(jnp.bfloat16).astype(jnp.float32), axis=0, keepdims=True
        )
        dprob = dot(values, d_c, 1, 1)
        dscore = (probs * (dprob - delta)).astype(jnp.bfloat16)
        ds_all[:, span] = dscore
        dq = (dot(keys, dscore, 0, 0) * factor).T
        for i in range(cols // BLK):
            g = c // BLK + i
            scale = power(qexp[g % blocks, g // blocks], width)
            dq_ref[g * BLK : (g + 1) * BLK, :] = (
                dq[i * BLK : (i + 1) * BLK] * scale
            ).astype(jnp.bfloat16)
    dk = dot(ds_all[...], q[...], 1, 0) * factor
    dv = dot(p_all[...], d[...], 1, 0)
    own_ref[:, :width] = dk[:rows]
    own_ref[:, width:] = dv[:rows]
    at = rows
    for mine_ref in mine_refs:
        end = at + mine_ref.shape[0]
        mine_ref[:, :width] = dk[at:end]
        mine_ref[:, width:] = dv[at:end]
        at = end
    other_ref[:, :width] = dk[at:].astype(jnp.bfloat16)
    other_ref[:, width:] = dv[at:].astype(jnp.bfloat16)


def make_on_device(sizes):
    heads_n, outers, inners = sizes
    steps, shared = plan(heads_n, inners)
    vmem = pl.BlockSpec(memory_space=pltpu.VMEM)
    hbm = pl.BlockSpec(memory_space=pltpu.HBM)
    keep = lambda a: pltpu.with_memory_space_constraint(a, pltpu.VMEM)
    stay = lambda a: pltpu.with_memory_space_constraint(a, pltpu.HBM)
    params = pltpu.CompilerParams(vmem_limit_bytes=24 * 1024 * 1024)

    def on_device(
        query_mant, key_mant, value_mant, out_grad, query_exp, key_exp, value_exp, block_order
    ):
        heads_out, rows, width = query_mant.shape
        kv_count = key_mant.shape[0]
        wide = 2 * width
        half = rows // 2
        count = heads_out * rows
        outer_at = lax.axis_index("outer")
        core = outer_at % 2
        kv_index = outer_at * heads_out // GROUP
        pick = lambda a: lax.dynamic_slice_in_dim(a, kv_index, 1, 0) if kv_count > 1 else a
        share = 0 if shared is None else 1
        zero = jnp.int32(0)
        spare = width - rows // BLK
        exps = lax.pad(pick(key_exp), zero, ((0, 7, 0), (0, spare, 0))) + lax.pad(
            pick(value_exp), zero, ((1, 6, 0), (0, spare, 0))
        )
        block, factors, *part = pl.pallas_call(
            lambda *refs: block_body(share, *refs),
            in_specs=[hbm] * 3,
            out_specs=[vmem] * (2 + share),
            out_shape=[
                pltpu.VMEM((rows, wide), jnp.bfloat16),
                pltpu.VMEM((rows // BLK, wide), jnp.float32),
                pltpu.VMEM((half, wide), jnp.bfloat16),
            ][: 2 + share],
            scratch_shapes=[
                pltpu.VMEM((1, rows, width), jnp.bfloat16),
                pltpu.VMEM((1, rows, width), jnp.bfloat16),
                pltpu.VMEM((8, width), jnp.int32),
                pltpu.SemaphoreType.DMA((3,)),
            ],
            compiler_params=params,
            name="scale_block",
        )(stay(pick(key_mant)), stay(pick(value_mant)), stay(exps))
        last = [lax.ppermute(p, ALL, moves(sizes, (shared, shared), False)) for p in part]
        mine = [lax.ppermute(block, ALL, moves(sizes, pair, False)) for pair in steps] + last
        other = [lax.ppermute(piece, "outer", flip(outers, 1)) for piece in mine]

        pieces = [block] + mine + other
        total = sum(p.shape[0] for p in pieces)
        held = sum(p.shape[0] for p in mine)
        out, dq, own_term, *mine_terms, other_term = pl.pallas_call(
            lambda *refs: attention_body(sizes, steps, shared, rows, len(pieces), *refs),
            in_specs=[hbm] * 4 + [vmem] * len(pieces),
            out_specs=[vmem] * (4 + len(mine)),
            out_shape=[
                jax.ShapeDtypeStruct((count, width), jnp.bfloat16),
                jax.ShapeDtypeStruct((count, width), jnp.bfloat16),
                pltpu.VMEM((rows, wide), jnp.float32),
            ]
            + [pltpu.VMEM(p.shape, jnp.float32) for p in mine]
            + [pltpu.VMEM((held, wide), jnp.bfloat16)],
            scratch_shapes=[
                pltpu.SMEM(block_order.shape, jnp.int32),
                pltpu.SMEM((rows // BLK, heads_out), jnp.int32),
                pltpu.VMEM((count, width), jnp.bfloat16),
                pltpu.VMEM((count, width), jnp.bfloat16),
                pltpu.SemaphoreType.DMA((4,)),
                pltpu.VMEM((total, wide), jnp.bfloat16),
                pltpu.VMEM((count, width), jnp.bfloat16),
                pltpu.VMEM((total, count), jnp.bfloat16),
                pltpu.VMEM((total, count), jnp.bfloat16),
            ],
            compiler_params=pltpu.CompilerParams(vmem_limit_bytes=48 * 1024 * 1024),
            name="attention",
        )(
            stay(block_order),
            stay(query_exp.T),
            stay(query_mant.reshape(count, width)),
            stay(out_grad.reshape(count, width)),
            *[keep(piece) for piece in pieces],
        )
        output = out.reshape(heads_out, rows, width)
        query_grad = dq.reshape(heads_out, rows, width)

        from_core = lax.ppermute(other_term, "outer", flip(outers, 1))
        pair_sums = []
        at = 0
        for term in mine_terms:
            end = at + term.shape[0]
            pair_sums.append((term + from_core[at:end].astype(jnp.float32)).astype(jnp.bfloat16))
            at = end
        summed = own_term
        if share:
            got = lax.ppermute(
                pair_sums[-1], ALL, moves(sizes, (shared, shared), True)
            ).astype(jnp.float32)
            none = jnp.zeros_like(got)
            low = jnp.concatenate([got, none], axis=0)
            high = jnp.concatenate([none, got], axis=0)
            summed = summed + jnp.where(core == 0, low, high)
        for pair, piece in zip(steps, pair_sums):
            got = lax.ppermute(piece, ALL, moves(sizes, pair, True))
            summed = summed + got.astype(jnp.float32)
        low = summed.astype(jnp.bfloat16)
        if kv_count == 1 and outers & (outers - 1) == 0:
            bit = outers // 2
            while bit:
                got = lax.ppermute(low, "outer", flip(outers, bit))
                summed = low.astype(jnp.float32) + got.astype(jnp.float32)
                low = summed.astype(jnp.bfloat16)
                bit //= 2
            grads = [
                (
                    summed[:, at : at + width].reshape(rows // BLK, BLK, width)
                    * factors[:, None, at : at + width]
                )
                .astype(jnp.bfloat16)
                .reshape(1, rows, width)
                for at in (0, width)
            ]
            return (output, query_grad, grads[0], grads[1])
        members = lax.all_gather(low, "outer", axis=0)
        summed = jnp.sum(
            members.astype(jnp.float32).reshape(kv_count, outers // kv_count, rows, wide), axis=1
        )
        key_grad = scaled(summed[:, :, :width].astype(jnp.bfloat16), key_exp)
        value_grad = scaled(summed[:, :, width:].astype(jnp.bfloat16), value_exp)
        return (output, query_grad, key_grad, value_grad)

    return on_device


def solution(mesh):
    sizes = (mesh.shape["head"], mesh.shape["outer"], mesh.shape["inner"])
    placed = (
        P("outer", ("head", "inner"), None),
        P(None, ("head", "inner"), None),
        P(None, ("head", "inner"), None),
        P("outer", ("head", "inner"), None),
        P("outer", ("head", "inner")),
        P(None, ("head", "inner")),
        P(None, ("head", "inner")),
        P(),
    )
    return jax.shard_map(
        make_on_device(sizes),
        mesh=mesh,
        in_specs=placed,
        out_specs=(
            P("outer", ("head", "inner"), None),
            P("outer", ("head", "inner"), None),
            P(None, ("head", "inner"), None),
            P(None, ("head", "inner"), None),
        ),
        check_vma=False,
    )
```
